32 devices in a mesh: gx: 4 (over y, core), gy: 4 (over z), gz: 2 (over x).
Axes of the slice: x: 2, y: 2, z: 4, core: 2. Of those that a mesh axis runs over, the one named last changes fastest.
Arguments:
- a_vals: float32 [4, 8, 2, 6, 128, 128], P('gy', 'gx', 'gz'), may hold values from -0.25 to 0.25
- a_cols: int32 [4, 8, 2, 6], P('gy', 'gx', 'gz'), may hold values from 0 to 15, as said below
- a_count: int32 [4, 8, 2], P('gy', 'gx', 'gz'), may hold values from 1 to 6, as said below
- p_vals: float32 [2, 16, 4, 1, 128, 128], P('gz', 'gy', 'gx'), may hold values from -6 to 6
- p_cols: int32 [2, 16, 4, 1], P('gz', 'gy', 'gx'), may hold values from 0 to 1, as said below
- p_count: int32 [2, 16, 4], P('gz', 'gy', 'gx'), may hold values from 0 to 1, as said below
Outputs:
- c_tiles: float32 [4096, 1024], P(('gy', 'gz'), 'gx')
The draws below stay inside these ranges and needn't reach their ends.
Inputs may be any that keep to these rules, and one draw needn't show every extreme that they name: `a_cols`: inner tile indices of one block row and slice are distinct across its 6 slots. Slots 0 to a_count - 1 are live; the block rows of every device include one with all 6 slots live. `p_cols`: column tiles of one block row and group are distinct across its 1 slots. Slots 0 to p_count - 1 are live; the block rows of every device include one with all 1 slots live.
All inputs are finite; a program needn't handle non-finite values.
Results may differ from the reference program's by a relative error of at most 0.0003.
Values sent between devices are 32-bit elements; how exact they have to be, the bound alone decides.
A program may use at most 128 MiB of HBM per device.

```python
import jax
import jax.numpy as jnp
from jax import lax

TILE = 128
ROWS_DEV = 2
SLOTS_A = 6
SLOTS_P = 1
COLS_DEV = 2
RX = 8
KZ = 16
N_GX = 4
N_GY = 4
N_GZ = 2


def draw_a_count(key, part):
    first = jax.random.randint(jax.random.fold_in(key, 11), (N_GY, RX, N_GZ), 1, SLOTS_A + 1)
    second = jax.random.randint(jax.random.fold_in(key, 12), (N_GY, RX, N_GZ), 1, SLOTS_A + 1)
    counts = jnp.minimum(first, second)
    picked = jax.random.randint(jax.random.fold_in(key, 13), (N_GY, RX // ROWS_DEV, 1, N_GZ), 0, ROWS_DEV)
    position = jnp.arange(ROWS_DEV, dtype=jnp.int32)[None, None, :, None]
    filled = (position == picked).reshape(N_GY, RX, N_GZ)
    return jnp.where(filled, SLOTS_A, counts).astype(jnp.int32)


def draw_a_cols(key, part):
    line_total = N_GY * RX * N_GZ
    base = jnp.broadcast_to(jnp.arange(KZ, dtype=jnp.int32), (line_total, KZ))
    mixed = jax.random.permutation(jax.random.fold_in(key, 21), base, axis=1, independent=True)
    return mixed[:, :SLOTS_A].reshape(N_GY, RX, N_GZ, SLOTS_A).astype(jnp.int32)


def draw_p_count(key, part):
    counts = jax.random.randint(jax.random.fold_in(key, 31), (N_GZ, KZ, N_GX), 0, SLOTS_P + 1)
    block_rows = KZ // N_GY
    picked = jax.random.randint(jax.random.fold_in(key, 32), (N_GZ, N_GY, 1, N_GX), 0, block_rows)
    position = jnp.arange(block_rows, dtype=jnp.int32)[None, None, :, None]
    filled = (position == picked).reshape(N_GZ, KZ, N_GX)
    return jnp.where(filled, SLOTS_P, counts).astype(jnp.int32)


def draw_p_cols(key, part):
    line_total = N_GZ * KZ * N_GX
    base = jnp.broadcast_to(jnp.arange(COLS_DEV, dtype=jnp.int32), (line_total, COLS_DEV))
    mixed = jax.random.permutation(jax.random.fold_in(key, 41), base, axis=1, independent=True)
    return mixed[:, :SLOTS_P].reshape(N_GZ, KZ, N_GX, SLOTS_P).astype(jnp.int32)


def shard_levels(rng, dims, cuts, least, largest):
    loudness = 1.0
    for dim, blocks in cuts:
        steps = jax.random.uniform(jax.random.fold_in(jax.random.fold_in(rng, 6), dim), (blocks,), jnp.float32, least / len(cuts), largest / len(cuts))
        loudness = loudness * jnp.repeat(jnp.exp(steps), dims[dim] // blocks).reshape((-1,) + (1,) * (len(dims) - 1 - dim))
    return loudness


def noise(own_key, shape, width, bound, cuts=(), kind=jnp.bfloat16):
    values = width * jax.random.normal(own_key, shape, jnp.float32)
    if cuts:
        values = values * shard_levels(own_key, shape, cuts, -0.22, 0.18)
    return jnp.clip(values, -bound, bound).astype(kind)


def setup_inputs(seed: int = 0) -> dict:
    key_of = jax.random.split(jax.random.key(seed), 7)
    a_vals = noise(key_of[0], (N_GY, RX, N_GZ, SLOTS_A, TILE, TILE), (4 * TILE) ** -0.5, 0.25, ((0, 4), (1, 4), (2, 2)), jnp.float32)
    a_cols = draw_a_cols(jax.random.fold_in(key_of[6], 71), 0)
    a_count = draw_a_count(jax.random.fold_in(key_of[6], 71), 0)
    p_vals = noise(key_of[3], (N_GZ, KZ, N_GX, SLOTS_P, TILE, TILE), 1.0, 6.0, ((0, 2), (1, 4), (2, 4)), jnp.float32)
    p_cols = draw_p_cols(jax.random.fold_in(key_of[6], 71), 0)
    p_count = draw_p_count(jax.random.fold_in(key_of[6], 71), 0)
    return dict(a_vals=a_vals, a_cols=a_cols, a_count=a_count, p_vals=p_vals, p_cols=p_cols, p_count=p_count)


def reference(a_vals, a_cols, a_count, p_vals, p_cols, p_count):
    tile_size = a_vals.shape[-1]
    groups_y, rows_x, slices, slots_a = a_cols.shape
    inner_rows = p_cols.shape[1]
    groups_x = p_cols.shape[2]
    slots_p = p_cols.shape[3]
    rows_all = groups_y * rows_x
    a_values = a_vals.reshape(rows_all, slices, slots_a, tile_size, tile_size)
    a_columns = a_cols.reshape(rows_all, slices, slots_a)
    a_counts = a_count.reshape(rows_all, slices)
    p_values = p_vals.reshape(slices * inner_rows, groups_x, slots_p, tile_size, tile_size)
    alive_p = jnp.arange(slots_p, dtype=jnp.int32) < p_count[..., None]
    matches = p_cols[..., None] == jnp.arange(COLS_DEV, dtype=jnp.int32)
    p_weights = (alive_p[..., None] & matches).astype(jnp.float32)
    p_weights = p_weights.reshape(slices * inner_rows, groups_x, slots_p, COLS_DEV)
    offsets = (jnp.arange(slices, dtype=jnp.int32) * inner_rows)[:, None]

    def one_row(row_index):
        alive_a = jnp.arange(slots_a, dtype=jnp.int32) < a_counts[row_index][:, None]
        tile_part = jnp.where(alive_a[..., None, None], a_values[row_index], 0.0)
        indices = a_columns[row_index].astype(jnp.int32) + offsets
        chosen = p_values[indices]
        weights = p_weights[indices]
        product = jnp.einsum("zsij,zsxpjk->zsxpik", tile_part, chosen, precision=lax.Precision.HIGHEST)
        placed = jnp.einsum("zsxpc,zsxpik->ixck", weights, product, precision=lax.Precision.HIGHEST)
        return placed.reshape(tile_size, groups_x * COLS_DEV * tile_size)

    result = lax.map(one_row, jnp.arange(rows_all, dtype=jnp.int32))
    return result.reshape(rows_all * tile_size, groups_x * COLS_DEV * tile_size)
```

```python
import functools

import jax
import jax.numpy as jnp
from jax import lax
from jax.experimental import pallas as pl
from jax.experimental.pallas import tpu as pltpu
from jax.sharding import PartitionSpec as P

COLS_DEV = 2
MESH = pl.DeviceIdType.MESH


def kernel(
    gx, gy, gz,
    a_ref, p_ref, m_ref, o_ref,
    a_all, p_all, ma, mp, sa, sp, p_hi, p_lo, c_send, c_recv,
    a_recv, a_sy, a_sp, a_sf, p_recv, p_send, ma_recv, ma_send, mp_recv, mp_send, s_sem,
    c_rs, c_ss,
):
    rows, slots, tile = a_ref.shape[0], a_ref.shape[1], a_ref.shape[2]
    inner, slots_p = p_ref.shape[0], p_ref.shape[1]
    rows_all = gx * rows
    rows_out = rows_all // gz
    zero_tile = gy * inner
    cuts_a = 2 if slots % 2 == 0 else 1
    cuts_p = 2 if inner % 2 == 0 else 1
    part_a, part_p = slots // cuts_a, inner // cuts_p
    me_x, me_y, me_z = lax.axis_index("gx"), lax.axis_index("gy"), lax.axis_index("gz")
    chips = gx // 2
    chip, core = me_x // 2, me_x % 2
    partner = chip * 2 + (1 - core)

    barrier = pltpu.get_barrier_semaphore()
    for name, size, me in (("gx", gx, me_x), ("gy", gy, me_y), ("gz", gz, me_z)):
        for d in range(1, size):
            pl.semaphore_signal(
                barrier, inc=1, device_id={name: lax.rem(me + d, size)}, device_id_type=MESH
            )
    local = []
    for r in range(rows):
        for h in range(cuts_a):
            cut = pl.ds(h * part_a, part_a)
            local.append(pltpu.make_async_copy(
                a_ref.at[r, cut], a_all.at[me_x, r, cut], a_recv.at[me_x, r, h]))
    for h in range(cuts_p):
        cut = pl.ds(h * part_p, part_p)
        local.append(pltpu.make_async_copy(
            p_ref.at[cut], p_all.at[me_y, cut], p_recv.at[me_y, h]))
    local.append(pltpu.make_async_copy(m_ref, ma.at[me_x], ma_recv.at[me_x]))
    local.append(pltpu.make_async_copy(m_ref, mp.at[me_y], mp_recv.at[me_y]))
    for copy in local:
        copy.start()
    pl.semaphore_wait(barrier, gx + gy + gz - 3)

    def remote(src, dst, send, recv, where):
        return pltpu.make_async_remote_copy(
            src_ref=src, dst_ref=dst, send_sem=send, recv_sem=recv,
            device_id=where, device_id_type=MESH)

    sends = []
    for d in range(1, gx):
        sends.append(remote(m_ref, ma.at[me_x], ma_send.at[d], ma_recv.at[me_x],
                            {"gx": lax.rem(me_x + d, gx)}))
    for d in range(1, gy):
        sends.append(remote(m_ref, mp.at[me_y], mp_send.at[d], mp_recv.at[me_y],
                            {"gy": lax.rem(me_y + d, gy)}))
    for r in range(rows):
        for h in range(cuts_a):
            cut = pl.ds(h * part_a, part_a)
            for d in range(1, chips):
                sends.append(remote(
                    a_ref.at[r, cut], a_all.at[me_x, r, cut], a_sy.at[d, r, h],
                    a_recv.at[me_x, r, h], {"gx": lax.rem(chip + d, chips) * 2 + core}))
            sends.append(remote(
                a_ref.at[r, cut], a_all.at[me_x, r, cut], a_sp.at[r, h],
                a_recv.at[me_x, r, h], {"gx": partner}))
    for copy in sends:
        copy.start()

    def p_copy(side, src, h, own):
        cut = pl.ds(h * part_p, part_p)
        source = p_ref.at[cut] if own else p_all.at[src, cut]
        step = 1 if side == 0 else -1
        return remote(source, p_all.at[src, cut], p_send.at[side, src, h],
                      p_recv.at[src, h], {"gy": lax.rem(me_y + step + gy, gy)})

    has_next = (me_y + 1 < gy, me_y >= 1)
    for h in range(cuts_p):
        for side in (0, 1):
            @pl.when(has_next[side])
            def _(side=side, h=h):
                p_copy(side, me_y, h, True).start()

    def wait_p(src, h):
        ref = p_all.at[src, pl.ds(h * part_p, part_p)]
        pltpu.make_async_copy(ref, ref, p_recv.at[src, h]).wait()

    def wait_a(g, r, h):
        ref = a_all.at[g, r, pl.ds(h * part_a, part_a)]
        pltpu.make_async_copy(ref, ref, a_recv.at[g, r, h]).wait()

    def split(src):
        pltpu.make_async_copy(mp.at[src], mp.at[src], mp_recv.at[src]).wait()
        copy = pltpu.make_async_copy(mp.at[src], sp.at[src], s_sem)
        copy.start()
        copy.wait()

        def one(k, carry):
            for c in range(COLS_DEV):
                value = jnp.zeros((tile, tile), jnp.float32)
                for s in range(slots_p):
                    code = sp[src, 1, k * slots_p + s]
                    value = value + jnp.where(code == c, p_all[src, k, s], 0.0)
                high = value.astype(jnp.bfloat16)
                low = (value - high.astype(jnp.float32)).astype(jnp.bfloat16)
                p_hi[src * inner + k, :, c * tile:(c + 1) * tile] = high
                p_lo[src * inner + k, :, c * tile:(c + 1) * tile] = low
            return carry

        lax.fori_loop(0, inner, one, 0)

    p_hi[zero_tile] = jnp.zeros_like(p_hi[zero_tile])
    p_lo[zero_tile] = jnp.zeros_like(p_lo[zero_tile])
    for h in range(cuts_p):
        wait_p(me_y, h)
    split(me_y)
    for g in range(gx):
        pltpu.make_async_copy(ma.at[g], ma.at[g], ma_recv.at[g]).wait()
        copy = pltpu.make_async_copy(ma.at[g], sa.at[g], s_sem)
        copy.start()
        copy.wait()

    relays = [(d, r, h) for r in range(rows) for h in range(cuts_a) for d in range(1, chips)]

    def relay_copy(d, r, h):
        src = lax.rem(chip - d + chips, chips) * 2 + core
        cut = pl.ds(h * part_a, part_a)
        ref = a_all.at[src, r, cut]
        return src, remote(ref, ref, a_sf.at[d, r, h], a_recv.at[src, r, h], {"gx": partner})

    def relay(d, r, h):
        src, copy = relay_copy(d, r, h)
        wait_a(src, r, h)
        copy.start()

    steps = [(d, h) for d in range(1, gy) for h in range(cuts_p)]
    done = 0
    for i, (d, h) in enumerate(steps):
        for side in (0, 1):
            src = me_y - d if side == 0 else me_y + d
            there = src >= 0 if side == 0 else src < gy

            @pl.when(there)
            def _(src=src, side=side, h=h):
                wait_p(src, h)

                @pl.when(has_next[side])
                def _():
                    p_copy(side, src, h, False).start()

                if h == cuts_p - 1:
                    split(src)
        goal = (i + 1) * len(relays) // len(steps) if i + 1 < len(steps) else len(relays)
        while done < goal:
            relay(*relays[done])
            done += 1

    def product(q):
        g, r = q // rows, lax.rem(q, rows)
        picks = [sa[g, 0, r * slots + s] for s in range(slots)]
        values = jnp.concatenate([a_all[g, r, s] for s in range(slots)], axis=1)
        high = values.astype(jnp.bfloat16)
        low = (values - high.astype(jnp.float32)).astype(jnp.bfloat16)
        right = jnp.concatenate([p_hi[i] for i in picks], axis=0)
        rest = jnp.concatenate([p_lo[i] for i in picks], axis=0)
        dot = functools.partial(jnp.dot, preferred_element_type=jnp.float32)
        return dot(high, right) + (dot(low, right) + dot(high, rest))

    def await_row(q):
        g, r = q // rows, lax.rem(q, rows)
        mine = jnp.logical_and(g % 2 == core, g // 2 != chip)

        @pl.when(jnp.logical_not(mine))
        def _():
            for h in range(cuts_a):
                wait_a(g, r, h)

    def c_copy(d, i):
        owner = lax.rem(me_z + d, gz)
        return remote(c_send.at[d, i], c_recv.at[d, i], c_ss.at[d, i], c_rs.at[d, i],
                      {"gz": owner})

    for d in range(1, gz):
        def send_row(i, carry, d=d):
            q = lax.rem(me_z + d, gz) * rows_out + i
            await_row(q)
            c_send[d, i] = product(q)
            c_copy(d, i).start()
            return carry

        lax.fori_loop(0, rows_out, send_row, 0)

    def own_row(i, carry):
        q = me_z * rows_out + i
        await_row(q)
        o_ref[pl.ds(pl.multiple_of(i * tile, tile), tile), :] = product(q)
        return carry

    lax.fori_loop(0, rows_out, own_row, 0)

    for d in range(1, gz):
        def add_row(i, carry, d=d):
            pltpu.make_async_copy(c_recv.at[d, i], c_recv.at[d, i], c_rs.at[d, i]).wait()
            at = pl.ds(pl.multiple_of(i * tile, tile), tile)
            o_ref[at, :] = o_ref[at, :] + c_recv[d, i]
            return carry

        lax.fori_loop(0, rows_out, add_row, 0)

    for copy in sends:
        copy.wait_send()
    for d, r, h in relays:
        relay_copy(d, r, h)[1].wait_send()
    for side in (0, 1):
        for d in range(0, gy):
            src = me_y - d if side == 0 else me_y + d
            there = src >= 0 if side == 0 else src < gy

            @pl.when(jnp.logical_and(there, has_next[side]))
            def _(src=src, side=side, d=d):
                for h in range(cuts_p):
                    p_copy(side, src, h, d == 0).wait_send()
    for d in range(1, gz):
        def sent(i, carry, d=d):
            c_copy(d, i).wait_send()
            return carry

        lax.fori_loop(0, rows_out, sent, 0)


def body(gx, gy, gz, a_vals, a_cols, a_count, p_vals, p_cols, p_count):
    rows, slots, tile = a_vals.shape[1], a_vals.shape[3], a_vals.shape[-1]
    inner, slots_p = p_vals.shape[1], p_vals.shape[3]
    alive = jnp.arange(slots, dtype=jnp.int32) < a_count[0, :, 0][:, None]
    picks = jnp.where(alive, a_cols[0, :, 0], gy * inner).reshape(1, -1)
    alive_p = jnp.arange(slots_p, dtype=jnp.int32) < p_count[0, :, 0][:, None]
    codes = jnp.where(alive_p, p_cols[0, :, 0], -1).reshape(1, -1)
    pad = lambda v, at: jnp.pad(v, ((at, 7 - at), (0, 128 - v.shape[1])))
    meta = pad(picks, 0) + pad(codes, 1)
    rows_all = gx * rows
    rows_out = rows_all // gz
    strip = COLS_DEV * tile
    cuts_a = 2 if slots % 2 == 0 else 1
    cuts_p = 2 if inner % 2 == 0 else 1
    dma = pltpu.SemaphoreType.DMA
    any_spec = pl.BlockSpec(memory_space=pl.ANY)
    vmem_spec = pl.BlockSpec(memory_space=pltpu.VMEM)
    return pl.pallas_call(
        functools.partial(kernel, gx, gy, gz),
        out_shape=jax.ShapeDtypeStruct((rows_out * tile, strip), jnp.float32),
        in_specs=[any_spec, any_spec, any_spec],
        out_specs=vmem_spec,
        scratch_shapes=[
            pltpu.VMEM((gx, rows, slots, tile, tile), jnp.float32),
            pltpu.VMEM((gy, inner, slots_p, tile, tile), jnp.float32),
            pltpu.VMEM((gx, 8, 128), jnp.int32),
            pltpu.VMEM((gy, 8, 128), jnp.int32),
            pltpu.SMEM((gx, 8, 128), jnp.int32),
            pltpu.SMEM((gy, 8, 128), jnp.int32),
            pltpu.VMEM((gy * inner + 1, tile, strip), jnp.bfloat16),
            pltpu.VMEM((gy * inner + 1, tile, strip), jnp.bfloat16),
            pltpu.VMEM((gz, rows_out, tile, strip), jnp.float32),
            pltpu.VMEM((gz, rows_out, tile, strip), jnp.float32),
            dma((gx, rows, cuts_a)),
            dma((max(gx // 2, 1), rows, cuts_a)),
            dma((rows, cuts_a)),
            dma((max(gx // 2, 1), rows, cuts_a)),
            dma((gy, cuts_p)),
            dma((2, gy, cuts_p)),
            dma((gx,)),
            dma((gx,)),
            dma((gy,)),
            dma((gy,)),
            dma,
            dma((gz, rows_out)),
            dma((gz, rows_out)),
        ],
        compiler_params=pltpu.CompilerParams(collective_id=0, has_side_effects=True),
    )(a_vals[0, :, 0], p_vals[0, :, 0], meta)


def solution(mesh):
    placed = (
        P("gy", "gx", "gz", None, None, None),
        P("gy", "gx", "gz", None),
        P("gy", "gx", "gz"),
        P("gz", "gy", "gx", None, None, None),
        P("gz", "gy", "gx", None),
        P("gz", "gy", "gx"),
    )
    sizes = (mesh.shape["gx"], mesh.shape["gy"], mesh.shape["gz"])
    return jax.shard_map(
        functools.partial(body, *sizes),
        mesh=mesh, in_specs=placed, out_specs=P(("gy", "gz"), "gx"), check_vma=False,
    )
```

```python
import functools

import jax
import jax.numpy as jnp
from jax import lax
from jax.experimental import pallas as pl
from jax.experimental.pallas import tpu as pltpu
from jax.sharding import PartitionSpec as P

COLS_DEV = 2
MESH = pl.DeviceIdType.MESH


def kernel(
    gx, gy, gz, slots_p,
    a_ref, p_ref, ac_ref, an_ref, pc_ref, pn_ref, o_ref,
    a_all, p_own, p_all, ma, mp, sa, sp, p_mul, c_send, c_recv,
    a_recv, a_sy, a_sp, a_sf, p_load, p_recv, p_send,
    ma_recv, ma_send, mp_recv, mp_send, s_sem, c_rs, c_ss,
):
    rows, slots, tile = a_ref.shape[0], a_ref.shape[1], a_ref.shape[2]
    tiles_p = p_ref.shape[0]
    inner = tiles_p // slots_p
    pairs = p_all.shape[2]
    rows_all = gx * rows
    rows_out = rows_all // gz
    zero_tile = gy * inner
    half = tile // 2
    cuts_a = a_recv.shape[2]
    part_a = slots // cuts_a
    me_x, me_y, me_z = lax.axis_index("gx"), lax.axis_index("gy"), lax.axis_index("gz")
    chips = gx // 2
    chip, core = me_x // 2, me_x % 2
    partner = chip * 2 + (1 - core)

    barrier = pltpu.get_barrier_semaphore()
    for name, size, me in (("gx", gx, me_x), ("gy", gy, me_y), ("gz", gz, me_z)):
        for d in range(1, size):
            pl.semaphore_signal(
                barrier, inc=1, device_id={name: lax.rem(me + d, size)}, device_id_type=MESH
            )
    load = pltpu.make_async_copy(p_ref, p_own, p_load)
    load.start()
    for r in range(rows):
        for h in range(cuts_a):
            cut = pl.ds(h * part_a, part_a)
            pltpu.make_async_copy(
                a_ref.at[r, cut], a_all.at[me_x, r, cut], a_recv.at[me_x, r, h]).start()

    line = lax.broadcasted_iota(jnp.int32, (8, 128), 0)
    lane = lax.broadcasted_iota(jnp.int32, (8, 128), 1)
    meta = jnp.zeros((8, 128), jnp.int32)
    for r in range(rows):
        for s in range(slots):
            pick = jnp.where(s < an_ref[r], ac_ref[0, r, 0, s], zero_tile)
            meta = jnp.where((line == 0) & (lane == r * slots + s), pick, meta)
    for t in range(tiles_p):
        code = jnp.where(t % slots_p < pn_ref[t // slots_p], pc_ref[t], -1)
        meta = jnp.where((line == 1) & (lane == t), code, meta)
    ma[me_x] = meta
    mp[me_y] = meta
    p_mul[0, zero_tile] = jnp.zeros_like(p_mul[0, zero_tile])
    p_mul[1, zero_tile] = jnp.zeros_like(p_mul[1, zero_tile])

    left = lax.broadcasted_iota(jnp.int32, (tile, tile), 1) < half
    load.wait()
    for j in range(pairs):
        one, two = p_own[2 * j], p_own[min(2 * j + 1, tiles_p - 1)]
        p_all[me_y, 0, j] = jnp.where(left, one, pltpu.roll(two, half, 1))
        p_all[me_y, 1, j] = jnp.where(left, pltpu.roll(one, half, 1), two)

    pl.semaphore_wait(barrier, gx + gy + gz - 3)

    def remote(src, dst, send, recv, where):
        return pltpu.make_async_remote_copy(
            src_ref=src, dst_ref=dst, send_sem=send, recv_sem=recv,
            device_id=where, device_id_type=MESH)

    sends = []
    for d in range(1, gx):
        sends.append(remote(ma.at[me_x], ma.at[me_x], ma_send.at[d], ma_recv.at[me_x],
                            {"gx": lax.rem(me_x + d, gx)}))
    for d in range(1, gy):
        sends.append(remote(mp.at[me_y], mp.at[me_y], mp_send.at[d], mp_recv.at[me_y],
                            {"gy": lax.rem(me_y + d, gy)}))
    for r in range(rows):
        for h in range(cuts_a):
            cut = pl.ds(h * part_a, part_a)
            for d in range(1, chips):
                sends.append(remote(
                    a_ref.at[r, cut], a_all.at[me_x, r, cut], a_sy.at[d, r, h],
                    a_recv.at[me_x, r, h], {"gx": lax.rem(chip + d, chips) * 2 + core}))
            sends.append(remote(
                a_ref.at[r, cut], a_all.at[me_x, r, cut], a_sp.at[r, h],
                a_recv.at[me_x, r, h], {"gx": partner}))
    for copy in sends:
        copy.start()

    def p_copy(side, src, h, j):
        ref = p_all.at[src, h, j]
        step = 1 if side == 0 else -1
        return remote(ref, ref, p_send.at[side, src, h, j], p_recv.at[src, h, j],
                      {"gy": lax.rem(me_y + step + gy, gy)})

    has_next = (me_y + 1 < gy, me_y >= 1)

    def send_own(h):
        for j in range(pairs):
            for side in (0, 1):
                @pl.when(has_next[side])
                def _(side=side, j=j):
                    p_copy(side, me_y, h, j).start()

    send_own(0)

    def wait_a(g, r, h):
        ref = a_all.at[g, r, pl.ds(h * part_a, part_a)]
        pltpu.make_async_copy(ref, ref, a_recv.at[g, r, h]).wait()

    for d in range(1, gx):
        g = lax.rem(me_x + d, gx)
        pltpu.make_async_copy(ma.at[g], ma.at[g], ma_recv.at[g]).wait()
    for d in range(1, gy):
        g = lax.rem(me_y + d, gy)
        pltpu.make_async_copy(mp.at[g], mp.at[g], mp_recv.at[g]).wait()
    moves = [pltpu.make_async_copy(ma, sa, s_sem.at[0]), pltpu.make_async_copy(mp, sp, s_sem.at[1])]
    for copy in moves:
        copy.start()
    for copy in moves:
        copy.wait()

    side_of_lane = lax.broadcasted_iota(jnp.int32, (tile, tile), 1) // half

    def split(src, h):
        def one(k, carry):
            value = jnp.zeros((tile, tile), jnp.float32)
            for s in range(slots_p):
                t = k * slots_p + s
                code = sp[src, 1, t]
                packed = p_all[src, h, t // 2]
                turned = pltpu.roll(packed, half, 1)
                placed = jnp.where(code == t % 2, packed, turned)
                value = value + jnp.where(side_of_lane == code, placed, 0.0)
            high = value.astype(jnp.bfloat16)
            low = (value - high.astype(jnp.float32)).astype(jnp.bfloat16)
            p_mul[h, src * inner + k, :, :tile] = high
            p_mul[h, src * inner + k, :, tile:] = low
            return carry

        lax.fori_loop(0, inner, one, 0)

    def relay_copy(d, r, h):
        src = lax.rem(chip - d + chips, chips) * 2 + core
        ref = a_all.at[src, r, pl.ds(h * part_a, part_a)]
        return src, remote(ref, ref, a_sf.at[d, r, h], a_recv.at[src, r, h], {"gx": partner})

    def relay(d, r, h):
        src, copy = relay_copy(d, r, h)
        wait_a(src, r, h)
        copy.start()

    def source(side, d):
        src = me_y - d if side == 0 else me_y + d
        return src, src >= 0 if side == 0 else src < gy

    def gather_half(h, relays):
        done = 0
        for d in range(1, gy):
            for side in (0, 1):
                src, there = source(side, d)

                @pl.when(there)
                def _(src=src, side=side):
                    for j in range(pairs):
                        ref = p_all.at[src, h, j]
                        pltpu.make_async_copy(ref, ref, p_recv.at[src, h, j]).wait()

                        @pl.when(has_next[side])
                        def _(j=j):
                            p_copy(side, src, h, j).start()

                    split(src, h)
            if h == 0 and d == max(gy - 2, 1):
                send_own(1)
            goal = max(0, d - 1) * len(relays) // (gy - 1)
            while done < goal:
                relay(*relays[done])
                done += 1
        while done < len(relays):
            relay(*relays[done])
            done += 1

    relays = [(d, r, h) for r in range(rows) for h in range(cuts_a) for d in range(1, chips)]

    def product(q, h):
        g, r = q // rows, lax.rem(q, rows)
        picks = [sa[g, 0, r * slots + s] for s in range(slots)]
        values = jnp.concatenate([a_all[g, r, s] for s in range(slots)], axis=1)
        high = values.astype(jnp.bfloat16)
        low = (values - high.astype(jnp.float32)).astype(jnp.bfloat16)
        right = jnp.concatenate([p_mul[h, i] for i in picks], axis=0)
        out = jnp.dot(jnp.concatenate([high, low], axis=0), right,
                      preferred_element_type=jnp.float32)
        return out[:tile, :tile] + (out[:tile, tile:] + out[tile:, :tile] + out[tile:, tile:])

    def await_row(q):
        g, r = q // rows, lax.rem(q, rows)
        mine = jnp.logical_and(g % 2 == core, g // 2 != chip)

        @pl.when(jnp.logical_not(mine))
        def _():
            for h in range(cuts_a):
                wait_a(g, r, h)

    def c_copy(d, i, h):
        return remote(c_send.at[d, i, h], c_recv.at[d, i, h], c_ss.at[d, i, h],
                      c_rs.at[d, i, h], {"gz": lax.rem(me_z + d, gz)})

    def send_rows(lines, halves, first):
        for d in range(1, gz):
            def send_row(n, carry, d=d):
                i = lines[0] + n * (lines[1] - lines[0] if len(lines) > 1 else 1)
                q = lax.rem(me_z + d, gz) * rows_out + i
                if first:
                    await_row(q)
                for h in halves:
                    c_send[d, i, h] = product(q, h)
                    c_copy(d, i, h).start()
                return carry

            lax.fori_loop(0, len(lines), send_row, 0)

    early = list(range(0, rows_out, rows))
    split(me_y, 0)
    gather_half(0, [x for x in relays if x[1] == 0])
    send_rows(early, (0,), True)
    split(me_y, 1)
    gather_half(1, [x for x in relays if x[1] > 0])
    send_rows(early, (1,), False)
    for r in range(1, rows):
        late = list(range(r, rows_out, rows))
        if late:
            send_rows(late, (0, 1), True)

    def own_row(i, carry):
        q = me_z * rows_out + i
        await_row(q)
        for h in (0, 1):
            c_send[0, i, h] = product(q, h)
        return carry

    lax.fori_loop(0, rows_out, own_row, 0)

    def finish(i):
        halves = []
        for h in (0, 1):
            value = c_send[0, i, h]
            for d in range(1, gz):
                ref = c_recv.at[d, i, h]
                pltpu.make_async_copy(ref, ref, c_rs.at[d, i, h]).wait()
                value = value + c_recv[d, i, h]
            halves.append(value)
        one, two = halves
        at = pl.ds(i * tile, tile)
        o_ref[at, :tile] = jnp.where(left, one, pltpu.roll(two, half, 1))
        o_ref[at, tile:] = jnp.where(left, pltpu.roll(one, half, 1), two)

    for r in range(rows):
        for i in range(r, rows_out, rows):
            finish(i)

    for copy in sends:
        copy.wait_send()
    for d, r, h in relays:
        relay_copy(d, r, h)[1].wait_send()
    for side in (0, 1):
        for d in range(0, gy):
            src, there = source(side, d)

            @pl.when(jnp.logical_and(there, has_next[side]))
            def _(src=src, side=side):
                for h in (0, 1):
                    for j in range(pairs):
                        p_copy(side, src, h, j).wait_send()
    for d in range(1, gz):
        for i in range(rows_out):
            for h in (0, 1):
                c_copy(d, i, h).wait_send()


def body(gx, gy, gz, a_vals, a_cols, a_count, p_vals, p_cols, p_count):
    rows, slots, tile = a_vals.shape[1], a_vals.shape[3], a_vals.shape[-1]
    inner, slots_p = p_vals.shape[1], p_vals.shape[3]
    tiles_p = inner * slots_p
    pairs = (tiles_p + 1) // 2
    rows_out = gx * rows // gz
    cuts_a = 2 if slots % 2 == 0 else 1
    dma = pltpu.SemaphoreType.DMA
    any_spec = pl.BlockSpec(memory_space=pl.ANY)
    smem_spec = pl.BlockSpec(memory_space=pltpu.SMEM)
    return pl.pallas_call(
        functools.partial(kernel, gx, gy, gz, slots_p),
        out_shape=jax.ShapeDtypeStruct((rows_out * tile, COLS_DEV * tile), jnp.float32),
        in_specs=[any_spec] * 2 + [smem_spec] * 4,
        out_specs=pl.BlockSpec(memory_space=pltpu.VMEM),
        scratch_shapes=[
            pltpu.VMEM((gx, rows, slots, tile, tile), jnp.float32),
            pltpu.VMEM((tiles_p, tile, tile), jnp.float32),
            pltpu.VMEM((gy, 2, pairs, tile, tile), jnp.float32),
            pltpu.VMEM((gx, 8, 128), jnp.int32),
            pltpu.VMEM((gy, 8, 128), jnp.int32),
            pltpu.SMEM((gx, 8, 128), jnp.int32),
            pltpu.SMEM((gy, 8, 128), jnp.int32),
            pltpu.VMEM((2, gy * inner + 1, tile, 2 * tile), jnp.bfloat16),
            pltpu.VMEM((gz, rows_out, 2, tile, tile), jnp.float32),
            pltpu.VMEM((gz, rows_out, 2, tile, tile), jnp.float32),
            dma((gx, rows, cuts_a)),
            dma((max(gx // 2, 1), rows, cuts_a)),
            dma((rows, cuts_a)),
            dma((max(gx // 2, 1), rows, cuts_a)),
            dma,
            dma((gy, 2, pairs)),
            dma((2, gy, 2, pairs)),
            dma((gx,)),
            dma((gx,)),
            dma((gy,)),
            dma((gy,)),
            dma((2,)),
            dma((gz, rows_out, 2)),
            dma((gz, rows_out, 2)),
        ],
        compiler_params=pltpu.CompilerParams(collective_id=0, has_side_effects=True),
    )(
        a_vals[0, :, 0], p_vals.reshape(tiles_p, tile, tile),
        a_cols, a_count.reshape(-1), p_cols.reshape(-1), p_count.reshape(-1),
    )


def solution(mesh):
    placed = (
        P("gy", "gx", "gz", None, None, None),
        P("gy", "gx", "gz", None),
        P("gy", "gx", "gz"),
        P("gz", "gy", "gx", None, None, None),
        P("gz", "gy", "gx", None),
        P("gz", "gy", "gx"),
    )
    sizes = (mesh.shape["gx"], mesh.shape["gy"], mesh.shape["gz"])
    return jax.shard_map(
        functools.partial(body, *sizes),
        mesh=mesh, in_specs=placed, out_specs=P(("gy", "gz"), "gx"), check_vma=False,
    )
```

```python
import functools

import jax
import jax.numpy as jnp
from jax import lax
from jax.experimental import pallas as pl
from jax.experimental.pallas import tpu as pltpu
from jax.sharding import PartitionSpec as P

COLS_DEV = 2
MESH = pl.DeviceIdType.MESH


def kernel(
    gx, gy, gz, slots_p,
    a_ref, p_ref, ac_hbm, an_hbm, pc_hbm, pn_hbm, o_ref,
    ac_ref, an_ref, pc_ref, pn_ref, i_load, a_all, p_own, p_all, ma, mp, sa, sp, p_mul, c_send, c_recv,
    a_recv, a_sy, a_sp, a_sf, p_load, p_recv, p_send,
    ma_recv, ma_send, mp_recv, mp_send, s_sem, c_rs, c_ss,
):
    rows, slots, tile = a_ref.shape[0], a_ref.shape[1], a_ref.shape[2]
    tiles_p = p_ref.shape[0]
    inner = tiles_p // slots_p
    pairs = p_all.shape[2]
    rows_all = gx * rows
    rows_out = rows_all // gz
    zero_tile = gy * inner
    half = tile // 2
    cuts_a = a_recv.shape[2]
    part_a = slots // cuts_a
    me_x, me_y, me_z = lax.axis_index("gx"), lax.axis_index("gy"), lax.axis_index("gz")
    chips = gx // 2
    chip, core = me_x // 2, me_x % 2
    partner = chip * 2 + (1 - core)

    barrier = pltpu.get_barrier_semaphore()
    for name, size, me in (("gx", gx, me_x), ("gy", gy, me_y), ("gz", gz, me_z)):
        for d in range(1, size):
            pl.semaphore_signal(
                barrier, inc=1, device_id={name: lax.rem(me + d, size)}, device_id_type=MESH
            )
    load = pltpu.make_async_copy(p_ref, p_own, p_load)
    load.start()
    small = [
        pltpu.make_async_copy(src, dst, i_load.at[n])
        for n, (src, dst) in enumerate((
            (ac_hbm, ac_ref), (an_hbm, an_ref), (pc_hbm, pc_ref), (pn_hbm, pn_ref)))
    ]
    for copy in small:
        copy.start()
    for r in range(rows):
        for h in range(cuts_a):
            cut = pl.ds(h * part_a, part_a)
            pltpu.make_async_copy(
                a_ref.at[r, cut], a_all.at[me_x, r, cut], a_recv.at[me_x, r, h]).start()

    pl.semaphore_wait(barrier, gx + gy + gz - 3)

    def remote(src, dst, send, recv, where):
        return pltpu.make_async_remote_copy(
            src_ref=src, dst_ref=dst, send_sem=send, recv_sem=recv,
            device_id=where, device_id_type=MESH)

    sends = []
    for r in range(rows):
        for h in range(cuts_a):
            cut = pl.ds(h * part_a, part_a)
            for d in range(1, chips):
                sends.append(remote(
                    a_ref.at[r, cut], a_all.at[me_x, r, cut], a_sy.at[d, r, h],
                    a_recv.at[me_x, r, h], {"gx": lax.rem(chip + d, chips) * 2 + core}))
            sends.append(remote(
                a_ref.at[r, cut], a_all.at[me_x, r, cut], a_sp.at[r, h],
                a_recv.at[me_x, r, h], {"gx": partner}))
    for copy in sends:
        copy.start()
    large = len(sends)

    left = lax.broadcasted_iota(jnp.int32, (tile, tile), 1) < half
    load.wait()
    for j in range(pairs):
        one, two = p_own[2 * j], p_own[min(2 * j + 1, tiles_p - 1)]
        p_all[me_y, 0, j] = jnp.where(left, one, pltpu.roll(two, half, 1))
        p_all[me_y, 1, j] = jnp.where(left, pltpu.roll(one, half, 1), two)

    def p_copy(side, src, h, j):
        ref = p_all.at[src, h, j]
        step = 1 if side == 0 else -1
        return remote(ref, ref, p_send.at[side, src, h, j], p_recv.at[src, h, j],
                      {"gy": lax.rem(me_y + step + gy, gy)})

    has_next = (me_y + 1 < gy, me_y >= 1)

    def send_own(h):
        for j in range(pairs):
            for side in (0, 1):
                @pl.when(has_next[side])
                def _(side=side, j=j):
                    p_copy(side, me_y, h, j).start()

    send_own(0)

    for copy in small:
        copy.wait()
    line = lax.broadcasted_iota(jnp.int32, (8, 128), 0)
    lane = lax.broadcasted_iota(jnp.int32, (8, 128), 1)
    meta = jnp.zeros((8, 128), jnp.int32)
    for r in range(rows):
        for s in range(slots):
            pick = jnp.where(s < an_ref[r], ac_ref[0, r, 0, s], zero_tile)
            meta = jnp.where((line == 0) & (lane == r * slots + s), pick, meta)
    for t in range(tiles_p):
        code = jnp.where(t % slots_p < pn_ref[t // slots_p], pc_ref[t], -1)
        meta = jnp.where((line == 1) & (lane == t), code, meta)
    ma[me_x] = meta
    mp[me_y] = meta
    p_mul[0, zero_tile] = jnp.zeros_like(p_mul[0, zero_tile])
    p_mul[1, zero_tile] = jnp.zeros_like(p_mul[1, zero_tile])

    for d in range(1, gx):
        sends.append(remote(ma.at[me_x], ma.at[me_x], ma_send.at[d], ma_recv.at[me_x],
                            {"gx": lax.rem(me_x + d, gx)}))
    for d in range(1, gy):
        sends.append(remote(mp.at[me_y], mp.at[me_y], mp_send.at[d], mp_recv.at[me_y],
                            {"gy": lax.rem(me_y + d, gy)}))
    for copy in sends[large:]:
        copy.start()

    def wait_a(g, r, h):
        ref = a_all.at[g, r, pl.ds(h * part_a, part_a)]
        pltpu.make_async_copy(ref, ref, a_recv.at[g, r, h]).wait()

    def indices():
        for d in range(1, gx):
            g = lax.rem(me_x + d, gx)
            pltpu.make_async_copy(ma.at[g], ma.at[g], ma_recv.at[g]).wait()
        for d in range(1, gy):
            g = lax.rem(me_y + d, gy)
            pltpu.make_async_copy(mp.at[g], mp.at[g], mp_recv.at[g]).wait()
        moves = [pltpu.make_async_copy(ma, sa, s_sem.at[0]), pltpu.make_async_copy(mp, sp, s_sem.at[1])]
        for copy in moves:
            copy.start()
        for copy in moves:
            copy.wait()

    side_of_lane = lax.broadcasted_iota(jnp.int32, (tile, tile), 1) // half

    def split(src, h):
        def one(k, carry):
            value = jnp.zeros((tile, tile), jnp.float32)
            for s in range(slots_p):
                t = k * slots_p + s
                code = sp[src, 1, t]
                packed = p_all[src, h, t // 2]
                turned = pltpu.roll(packed, half, 1)
                placed = jnp.where(code == t % 2, packed, turned)
                value = value + jnp.where(side_of_lane == code, placed, 0.0)
            high = value.astype(jnp.bfloat16)
            low = (value - high.astype(jnp.float32)).astype(jnp.bfloat16)
            p_mul[h, src * inner + k, :, :tile] = high
            p_mul[h, src * inner + k, :, tile:] = low
            return carry

        lax.fori_loop(0, inner, one, 0)

    def relay_copy(d, r, h):
        src = lax.rem(chip - d + chips, chips) * 2 + core
        ref = a_all.at[src, r, pl.ds(h * part_a, part_a)]
        return src, remote(ref, ref, a_sf.at[d, r, h], a_recv.at[src, r, h], {"gx": partner})

    def relay(d, r, h):
        src, copy = relay_copy(d, r, h)
        wait_a(src, r, h)
        copy.start()

    def source(side, d):
        src = me_y - d if side == 0 else me_y + d
        return src, src >= 0 if side == 0 else src < gy

    def gather_half(h, relays):
        done = 0
        for d in range(1, gy):
            for side in (0, 1):
                src, there = source(side, d)

                @pl.when(there)
                def _(src=src, side=side):
                    for j in range(pairs):
                        ref = p_all.at[src, h, j]
                        pltpu.make_async_copy(ref, ref, p_recv.at[src, h, j]).wait()

                        @pl.when(has_next[side])
                        def _(j=j):
                            p_copy(side, src, h, j).start()

            if d == 1:
                if h == 0:
                    indices()
                split(me_y, h)
            for side in (0, 1):
                src, there = source(side, d)

                @pl.when(there)
                def _(src=src):
                    split(src, h)

            if h == 0 and d == max(gy - 2, 1):
                send_own(1)
            goal = max(0, d - 1) * len(relays) // (gy - 1)
            while done < goal:
                relay(*relays[done])
                done += 1
        while done < len(relays):
            relay(*relays[done])
            done += 1

    relays = [(d, r, h) for r in range(rows) for h in range(cuts_a) for d in range(1, chips)]

    def product(q, h):
        g, r = q // rows, lax.rem(q, rows)
        picks = [sa[g, 0, r * slots + s] for s in range(slots)]
        values = jnp.concatenate([a_all[g, r, s] for s in range(slots)], axis=1)
        high = values.astype(jnp.bfloat16)
        low = (values - high.astype(jnp.float32)).astype(jnp.bfloat16)
        right = jnp.concatenate([p_mul[h, i] for i in picks], axis=0)
        out = jnp.dot(jnp.concatenate([high, low], axis=0), right,
                      preferred_element_type=jnp.float32)
        return out[:tile, :tile] + (out[:tile, tile:] + out[tile:, :tile] + out[tile:, tile:])

    def await_row(q):
        g, r = q // rows, lax.rem(q, rows)
        mine = jnp.logical_and(g % 2 == core, g // 2 != chip)

        @pl.when(jnp.logical_not(mine))
        def _():
            for h in range(cuts_a):
                wait_a(g, r, h)

    def c_copy(d, i, h):
        return remote(c_send.at[d, i, h], c_recv.at[d, i, h], c_ss.at[d, i, h],
                      c_rs.at[d, i, h], {"gz": lax.rem(me_z + d, gz)})

    def send_rows(lines, halves, first):
        for d in range(1, gz):
            def send_row(n, carry, d=d):
                i = lines[0] + n * (lines[1] - lines[0] if len(lines) > 1 else 1)
                q = lax.rem(me_z + d, gz) * rows_out + i
                if first:
                    await_row(q)
                for h in halves:
                    c_send[d, i, h] = product(q, h)
                    c_copy(d, i, h).start()
                return carry

            lax.fori_loop(0, len(lines), send_row, 0)

    early = list(range(0, rows_out, rows))
    gather_half(0, [x for x in relays if x[1] == 0])
    send_rows(early, (0,), True)
    gather_half(1, [x for x in relays if x[1] > 0])
    send_rows(early, (1,), False)
    for r in range(1, rows):
        late = list(range(r, rows_out, rows))
        if late:
            send_rows(late, (0, 1), True)

    def own_row(i, carry):
        q = me_z * rows_out + i
        await_row(q)
        for h in (0, 1):
            c_send[0, i, h] = product(q, h)
        return carry

    lax.fori_loop(0, rows_out, own_row, 0)

    def finish(i):
        halves = []
        for h in (0, 1):
            value = c_send[0, i, h]
            for d in range(1, gz):
                ref = c_recv.at[d, i, h]
                pltpu.make_async_copy(ref, ref, c_rs.at[d, i, h]).wait()
                value = value + c_recv[d, i, h]
            halves.append(value)
        one, two = halves
        at = pl.ds(i * tile, tile)
        o_ref[at, :tile] = jnp.where(left, one, pltpu.roll(two, half, 1))
        o_ref[at, tile:] = jnp.where(left, pltpu.roll(one, half, 1), two)

    for r in range(rows):
        for i in range(r, rows_out, rows):
            finish(i)

    for copy in sends:
        copy.wait_send()
    for d, r, h in relays:
        relay_copy(d, r, h)[1].wait_send()
    for side in (0, 1):
        for d in range(0, gy):
            src, there = source(side, d)

            @pl.when(jnp.logical_and(there, has_next[side]))
            def _(src=src, side=side):
                for h in (0, 1):
                    for j in range(pairs):
                        p_copy(side, src, h, j).wait_send()
    for d in range(1, gz):
        for i in range(rows_out):
            for h in (0, 1):
                c_copy(d, i, h).wait_send()


def body(gx, gy, gz, a_vals, a_cols, a_count, p_vals, p_cols, p_count):
    rows, slots, tile = a_vals.shape[1], a_vals.shape[3], a_vals.shape[-1]
    inner, slots_p = p_vals.shape[1], p_vals.shape[3]
    tiles_p = inner * slots_p
    pairs = (tiles_p + 1) // 2
    rows_out = gx * rows // gz
    cuts_a = 2 if slots % 2 == 0 else 1
    dma = pltpu.SemaphoreType.DMA
    any_spec = pl.BlockSpec(memory_space=pl.ANY)
    return pl.pallas_call(
        functools.partial(kernel, gx, gy, gz, slots_p),
        out_shape=jax.ShapeDtypeStruct((rows_out * tile, COLS_DEV * tile), jnp.float32),
        in_specs=[any_spec] * 6,
        out_specs=pl.BlockSpec(memory_space=pltpu.VMEM),
        scratch_shapes=[
            pltpu.SMEM(a_cols.shape, jnp.int32),
            pltpu.SMEM((rows,), jnp.int32),
            pltpu.SMEM((tiles_p,), jnp.int32),
            pltpu.SMEM((inner,), jnp.int32),
            dma((4,)),
            pltpu.VMEM((gx, rows, slots, tile, tile), jnp.float32),
            pltpu.VMEM((tiles_p, tile, tile), jnp.float32),
            pltpu.VMEM((gy, 2, pairs, tile, tile), jnp.float32),
            pltpu.VMEM((gx, 8, 128), jnp.int32),
            pltpu.VMEM((gy, 8, 128), jnp.int32),
            pltpu.SMEM((gx, 8, 128), jnp.int32),
            pltpu.SMEM((gy, 8, 128), jnp.int32),
            pltpu.VMEM((2, gy * inner + 1, tile, 2 * tile), jnp.bfloat16),
            pltpu.VMEM((gz, rows_out, 2, tile, tile), jnp.float32),
            pltpu.VMEM((gz, rows_out, 2, tile, tile), jnp.float32),
            dma((gx, rows, cuts_a)),
            dma((max(gx // 2, 1), rows, cuts_a)),
            dma((rows, cuts_a)),
            dma((max(gx // 2, 1), rows, cuts_a)),
            dma,
            dma((gy, 2, pairs)),
            dma((2, gy, 2, pairs)),
            dma((gx,)),
            dma((gx,)),
            dma((gy,)),
            dma((gy,)),
            dma((2,)),
            dma((gz, rows_out, 2)),
            dma((gz, rows_out, 2)),
        ],
        compiler_params=pltpu.CompilerParams(collective_id=0, has_side_effects=True),
    )(
        a_vals[0, :, 0], p_vals.reshape(tiles_p, tile, tile),
        a_cols, a_count.reshape(-1), p_cols.reshape(-1), p_count.reshape(-1),
    )


def solution(mesh):
    placed = (
        P("gy", "gx", "gz", None, None, None),
        P("gy", "gx", "gz", None),
        P("gy", "gx", "gz"),
        P("gz", "gy", "gx", None, None, None),
        P("gz", "gy", "gx", None),
        P("gz", "gy", "gx"),
    )
    sizes = (mesh.shape["gx"], mesh.shape["gy"], mesh.shape["gz"])
    return jax.shard_map(
        functools.partial(body, *sizes),
        mesh=mesh, in_specs=placed, out_specs=P(("gy", "gz"), "gx"), check_vma=False,
    )
```

```python
import functools

import jax
import jax.numpy as jnp
from jax import lax
from jax.experimental import pallas as pl
from jax.experimental.pallas import tpu as pltpu
from jax.sharding import PartitionSpec as P

COLS_DEV = 2
MESH = pl.DeviceIdType.MESH


def kernel(
    gx, gy, gz, slots_p,
    a_ref, p_ref, ac_hbm, an_hbm, pc_hbm, pn_hbm, o_ref,
    ac_ref, an_ref, pc_ref, pn_ref, i_load, a_all, p_own, p_all, ma, mp, sa, sp, p_mul, c_send, c_recv,
    a_recv, a_sy, a_sp, a_sf, p_load, p_recv, p_send,
    ma_recv, ma_send, mp_recv, mp_send, s_sem, c_rs, c_ss,
):
    rows, slots, tile = a_ref.shape[0], a_ref.shape[1], a_ref.shape[2]
    tiles_p = p_ref.shape[0]
    inner = tiles_p // slots_p
    pairs = p_all.shape[2]
    rows_all = gx * rows
    rows_out = rows_all // gz
    zero_tile = gy * inner
    half = tile // 2
    cuts_a = a_recv.shape[2]
    part_a = slots // cuts_a
    me_x, me_y, me_z = lax.axis_index("gx"), lax.axis_index("gy"), lax.axis_index("gz")
    chips = gx // 2
    chip, core = me_x // 2, me_x % 2
    partner = chip * 2 + (1 - core)

    barrier = pltpu.get_barrier_semaphore()
    for name, size, me in (("gx", gx, me_x), ("gy", gy, me_y), ("gz", gz, me_z)):
        for d in range(1, size):
            pl.semaphore_signal(
                barrier, inc=1, device_id={name: lax.rem(me + d, size)}, device_id_type=MESH
            )
    load = pltpu.make_async_copy(p_ref, p_own, p_load)
    load.start()
    small = [
        pltpu.make_async_copy(src, dst, i_load.at[n])
        for n, (src, dst) in enumerate((
            (ac_hbm, ac_ref), (an_hbm, an_ref), (pc_hbm, pc_ref), (pn_hbm, pn_ref)))
    ]
    for copy in small:
        copy.start()
    for r in range(rows):
        for h in range(cuts_a):
            cut = pl.ds(h * part_a, part_a)
            pltpu.make_async_copy(
                a_ref.at[r, cut], a_all.at[me_x, r, cut], a_recv.at[me_x, r, h]).start()

    pl.semaphore_wait(barrier, gx + gy + gz - 3)

    def remote(src, dst, send, recv, where):
        return pltpu.make_async_remote_copy(
            src_ref=src, dst_ref=dst, send_sem=send, recv_sem=recv,
            device_id=where, device_id_type=MESH)

    sends = []
    for r in range(rows):
        for h in range(cuts_a):
            cut = pl.ds(h * part_a, part_a)
            for d in range(1, chips):
                sends.append(remote(
                    a_ref.at[r, cut], a_all.at[me_x, r, cut], a_sy.at[d, r, h],
                    a_recv.at[me_x, r, h], {"gx": lax.rem(chip + d, chips) * 2 + core}))
            sends.append(remote(
                a_ref.at[r, cut], a_all.at[me_x, r, cut], a_sp.at[r, h],
                a_recv.at[me_x, r, h], {"gx": partner}))
    large = len(sends)
    first = large // rows
    for copy in sends[:first]:
        copy.start()

    left = lax.broadcasted_iota(jnp.int32, (tile, tile), 1) < half
    load.wait()
    for j in range(pairs):
        one, two = p_own[2 * j], p_own[min(2 * j + 1, tiles_p - 1)]
        p_all[me_y, 0, j] = jnp.where(left, one, pltpu.roll(two, half, 1))
        p_all[me_y, 1, j] = jnp.where(left, pltpu.roll(one, half, 1), two)

    def p_copy(side, src, h, j):
        ref = p_all.at[src, h, j]
        step = 1 if side == 0 else -1
        return remote(ref, ref, p_send.at[side, src, h, j], p_recv.at[src, h, j],
                      {"gy": lax.rem(me_y + step + gy, gy)})

    has_next = (me_y + 1 < gy, me_y >= 1)

    def send_own(h):
        for j in range(pairs):
            for side in (0, 1):
                @pl.when(has_next[side])
                def _(side=side, j=j):
                    p_copy(side, me_y, h, j).start()

    send_own(0)

    for copy in small:
        copy.wait()
    line = lax.broadcasted_iota(jnp.int32, (8, 128), 0)
    lane = lax.broadcasted_iota(jnp.int32, (8, 128), 1)
    meta = jnp.zeros((8, 128), jnp.int32)
    for r in range(rows):
        for s in range(slots):
            pick = jnp.where(s < an_ref[r], ac_ref[0, r, 0, s], zero_tile)
            meta = jnp.where((line == 0) & (lane == r * slots + s), pick, meta)
    for t in range(tiles_p):
        code = jnp.where(t % slots_p < pn_ref[t // slots_p], pc_ref[t], -1)
        meta = jnp.where((line == 1) & (lane == t), code, meta)
    ma[me_x] = meta
    mp[me_y] = meta
    p_mul[0, zero_tile] = jnp.zeros_like(p_mul[0, zero_tile])
    p_mul[1, zero_tile] = jnp.zeros_like(p_mul[1, zero_tile])

    for d in range(1, gx):
        sends.append(remote(ma.at[me_x], ma.at[me_x], ma_send.at[d], ma_recv.at[me_x],
                            {"gx": lax.rem(me_x + d, gx)}))
    for d in range(1, gy):
        sends.append(remote(mp.at[me_y], mp.at[me_y], mp_send.at[d], mp_recv.at[me_y],
                            {"gy": lax.rem(me_y + d, gy)}))
    for copy in sends[large:] + sends[first:large]:
        copy.start()

    def wait_a(g, r, h):
        ref = a_all.at[g, r, pl.ds(h * part_a, part_a)]
        pltpu.make_async_copy(ref, ref, a_recv.at[g, r, h]).wait()

    def indices(size, me, held, scalars, arrived, n):
        for d in range(1, size):
            g = lax.rem(me + d, size)
            pltpu.make_async_copy(held.at[g], held.at[g], arrived.at[g]).wait()
        copy = pltpu.make_async_copy(held, scalars, s_sem.at[n])
        copy.start()
        copy.wait()

    side_of_lane = lax.broadcasted_iota(jnp.int32, (tile, tile), 1) // half

    def split(src, h):
        def one(k, carry):
            value = jnp.zeros((tile, tile), jnp.float32)
            for s in range(slots_p):
                t = k * slots_p + s
                code = sp[src, 1, t]
                packed = p_all[src, h, t // 2]
                turned = pltpu.roll(packed, half, 1)
                placed = jnp.where(code == t % 2, packed, turned)
                value = value + jnp.where(side_of_lane == code, placed, 0.0)
            high = value.astype(jnp.bfloat16)
            low = (value - high.astype(jnp.float32)).astype(jnp.bfloat16)
            p_mul[h, src * inner + k, :, :tile] = high
            p_mul[h, src * inner + k, :, tile:] = low
            return carry

        lax.fori_loop(0, inner, one, 0)

    def relay_copy(d, r, h):
        src = lax.rem(chip - d + chips, chips) * 2 + core
        ref = a_all.at[src, r, pl.ds(h * part_a, part_a)]
        return src, remote(ref, ref, a_sf.at[d, r, h], a_recv.at[src, r, h], {"gx": partner})

    def relay(d, r, h):
        src, copy = relay_copy(d, r, h)
        wait_a(src, r, h)
        copy.start()

    def source(side, d):
        src = me_y - d if side == 0 else me_y + d
        return src, src >= 0 if side == 0 else src < gy

    def gather_half(h, relays):
        done = 0
        for d in range(1, gy):
            for side in (0, 1):
                src, there = source(side, d)

                @pl.when(there)
                def _(src=src, side=side):
                    for j in range(pairs):
                        ref = p_all.at[src, h, j]
                        pltpu.make_async_copy(ref, ref, p_recv.at[src, h, j]).wait()

                        @pl.when(has_next[side])
                        def _(j=j):
                            p_copy(side, src, h, j).start()

            if d == 1:
                if h == 0:
                    indices(gy, me_y, mp, sp, mp_recv, 1)
                split(me_y, h)
            for side in (0, 1):
                src, there = source(side, d)

                @pl.when(there)
                def _(src=src):
                    split(src, h)

            if h == 0 and d == max(gy - 2, 1):
                send_own(1)
            goal = max(0, d - 1) * len(relays) // (gy - 1)
            while done < goal:
                relay(*relays[done])
                done += 1
        while done < len(relays):
            relay(*relays[done])
            done += 1

    relays = [(d, r, h) for r in range(rows) for h in range(cuts_a) for d in range(1, chips)]

    def product(q, h):
        g, r = q // rows, lax.rem(q, rows)
        picks = [sa[g, 0, r * slots + s] for s in range(slots)]
        values = jnp.concatenate([a_all[g, r, s] for s in range(slots)], axis=1)
        high = values.astype(jnp.bfloat16)
        low = (values - high.astype(jnp.float32)).astype(jnp.bfloat16)
        right = jnp.concatenate([p_mul[h, i] for i in picks], axis=0)
        out = jnp.dot(jnp.concatenate([high, low], axis=0), right,
                      preferred_element_type=jnp.float32)
        return out[:tile, :tile] + (out[:tile, tile:] + out[tile:, :tile] + out[tile:, tile:])

    def await_row(q):
        g, r = q // rows, lax.rem(q, rows)
        mine = jnp.logical_and(g % 2 == core, g // 2 != chip)

        @pl.when(jnp.logical_not(mine))
        def _():
            for h in range(cuts_a):
                wait_a(g, r, h)

    def c_copy(d, i, h):
        return remote(c_send.at[d, i, h], c_recv.at[d, i, h], c_ss.at[d, i, h],
                      c_rs.at[d, i, h], {"gz": lax.rem(me_z + d, gz)})

    def send_rows(lines, halves, first):
        for d in range(1, gz):
            def send_row(n, carry, d=d):
                i = lines[0] + n * (lines[1] - lines[0] if len(lines) > 1 else 1)
                q = lax.rem(me_z + d, gz) * rows_out + i
                if first:
                    await_row(q)
                for h in halves:
                    c_send[d, i, h] = product(q, h)
                    c_copy(d, i, h).start()
                return carry

            lax.fori_loop(0, len(lines), send_row, 0)

    early = list(range(0, rows_out, rows))
    gather_half(0, [x for x in relays if x[1] == 0])
    indices(gx, me_x, ma, sa, ma_recv, 0)
    send_rows(early, (0,), True)
    gather_half(1, [x for x in relays if x[1] > 0])
    send_rows(early, (1,), False)
    for r in range(1, rows):
        late = list(range(r, rows_out, rows))
        if late:
            send_rows(late, (0, 1), True)

    def own_row(i, carry):
        q = me_z * rows_out + i
        await_row(q)
        for h in (0, 1):
            c_send[0, i, h] = product(q, h)
        return carry

    lax.fori_loop(0, rows_out, own_row, 0)

    def finish(i):
        halves = []
        for h in (0, 1):
            value = c_send[0, i, h]
            for d in range(1, gz):
                ref = c_recv.at[d, i, h]
                pltpu.make_async_copy(ref, ref, c_rs.at[d, i, h]).wait()
                value = value + c_recv[d, i, h]
            halves.append(value)
        one, two = halves
        at = pl.ds(i * tile, tile)
        o_ref[at, :tile] = jnp.where(left, one, pltpu.roll(two, half, 1))
        o_ref[at, tile:] = jnp.where(left, pltpu.roll(one, half, 1), two)

    for r in range(rows):
        for i in range(r, rows_out, rows):
            finish(i)

    for copy in sends:
        copy.wait_send()
    for d, r, h in relays:
        relay_copy(d, r, h)[1].wait_send()
    for side in (0, 1):
        for d in range(0, gy):
            src, there = source(side, d)

            @pl.when(jnp.logical_and(there, has_next[side]))
            def _(src=src, side=side):
                for h in (0, 1):
                    for j in range(pairs):
                        p_copy(side, src, h, j).wait_send()
    for d in range(1, gz):
        for i in range(rows_out):
            for h in (0, 1):
                c_copy(d, i, h).wait_send()


def body(gx, gy, gz, a_vals, a_cols, a_count, p_vals, p_cols, p_count):
    rows, slots, tile = a_vals.shape[1], a_vals.shape[3], a_vals.shape[-1]
    inner, slots_p = p_vals.shape[1], p_vals.shape[3]
    tiles_p = inner * slots_p
    pairs = (tiles_p + 1) // 2
    rows_out = gx * rows // gz
    cuts_a = 2 if slots % 2 == 0 else 1
    dma = pltpu.SemaphoreType.DMA
    any_spec = pl.BlockSpec(memory_space=pl.ANY)
    return pl.pallas_call(
        functools.partial(kernel, gx, gy, gz, slots_p),
        out_shape=jax.ShapeDtypeStruct((rows_out * tile, COLS_DEV * tile), jnp.float32),
        in_specs=[any_spec] * 6,
        out_specs=pl.BlockSpec(memory_space=pltpu.VMEM),
        scratch_shapes=[
            pltpu.SMEM(a_cols.shape, jnp.int32),
            pltpu.SMEM((rows,), jnp.int32),
            pltpu.SMEM((tiles_p,), jnp.int32),
            pltpu.SMEM((inner,), jnp.int32),
            dma((4,)),
            pltpu.VMEM((gx, rows, slots, tile, tile), jnp.float32),
            pltpu.VMEM((tiles_p, tile, tile), jnp.float32),
            pltpu.VMEM((gy, 2, pairs, tile, tile), jnp.float32),
            pltpu.VMEM((gx, 8, 128), jnp.int32),
            pltpu.VMEM((gy, 8, 128), jnp.int32),
            pltpu.SMEM((gx, 8, 128), jnp.int32),
            pltpu.SMEM((gy, 8, 128), jnp.int32),
            pltpu.VMEM((2, gy * inner + 1, tile, 2 * tile), jnp.bfloat16),
            pltpu.VMEM((gz, rows_out, 2, tile, tile), jnp.float32),
            pltpu.VMEM((gz, rows_out, 2, tile, tile), jnp.float32),
            dma((gx, rows, cuts_a)),
            dma((max(gx // 2, 1), rows, cuts_a)),
            dma((rows, cuts_a)),
            dma((max(gx // 2, 1), rows, cuts_a)),
            dma,
            dma((gy, 2, pairs)),
            dma((2, gy, 2, pairs)),
            dma((gx,)),
            dma((gx,)),
            dma((gy,)),
            dma((gy,)),
            dma((2,)),
            dma((gz, rows_out, 2)),
            dma((gz, rows_out, 2)),
        ],
        compiler_params=pltpu.CompilerParams(collective_id=0, has_side_effects=True),
    )(
        a_vals[0, :, 0], p_vals.reshape(tiles_p, tile, tile),
        a_cols, a_count.reshape(-1), p_cols.reshape(-1), p_count.reshape(-1),
    )


def solution(mesh):
    placed = (
        P("gy", "gx", "gz", None, None, None),
        P("gy", "gx", "gz", None),
        P("gy", "gx", "gz"),
        P("gz", "gy", "gx", None, None, None),
        P("gz", "gy", "gx", None),
        P("gz", "gy", "gx"),
    )
    sizes = (mesh.shape["gx"], mesh.shape["gy"], mesh.shape["gz"])
    return jax.shard_map(
        functools.partial(body, *sizes),
        mesh=mesh, in_specs=placed, out_specs=P(("gy", "gz"), "gx"), check_vma=False,
    )
```
